1024 devices in a mesh: dp: 8 (over y), expert: 8 (over z), tensor: 16 (over x, core).
Axes of the slice: x: 8, y: 8, z: 8, core: 2. Of those that a mesh axis runs over, the one named last changes fastest.
Arguments:
- grad_out: bfloat16 [8192, 6144], P(('dp', 'expert'), 'tensor'), may hold values from -0.1875 to 0.1875
- expert_ids: int32 [8192, 2], P(('dp', 'expert')), may hold values from 0 to 7, all different within a row; in each aligned block of 128 rows (0 to 127, 128 to 255, ...) at most 64 rows name the same one
- route_gates: float32 [8192, 2], P(('dp', 'expert')), may hold values from 0.1 to 1
- saved_hidden: bfloat16 [8, 2048, 16384], P('expert', 'dp', 'tensor'), may hold values from -6 to 6
Outputs:
- weight_grad: bfloat16 [8, 16384, 6144], P('expert', 'tensor', 'dp')
The draws below stay inside these ranges and needn't reach their ends.
Inputs may be any that keep to these rules, and one draw needn't show every extreme that they name: `expert_ids`: each row names 2 different experts. Among the rows of one device no expert is named by more than 64 rows, and every expert is named somewhere.
All inputs are finite; a program needn't handle non-finite values.
Results may differ from the reference program's by a relative error of at most 0.0049.
Values may be sent and summed in bfloat16 or wider, within the bound.
No kernel may reach another device: no remote copies, remote signals or barrier semaphores. Data moves between devices by JAX's collectives and lax.ppermute only.
A program may use at most 32 MiB of HBM per device.

```python
import math
import jax
import jax.numpy as jnp
import numpy as np
from jax import lax

D = 6144
FF = 16384
TOP = 2
TOK_DEV = 128
CAP = 32
EXPERTS = 8
TOKENS = 8192
SLOTS = 2048
N_DP = 8


def block_scale(key, dims, cuts, smallest, high):
    def one(position, shards_of):
        draws = jax.random.uniform(jax.random.fold_in(jax.random.fold_in(key, 6), position), (shards_of,), jnp.float32, smallest / len(cuts), high / len(cuts))
        return jnp.repeat(jnp.exp(draws), dims[position] // shards_of).reshape((-1,) + (1,) * (len(dims) - position - 1))

    gain = one(*cuts[0])
    for cut in cuts[1:]:
        gain = gain * one(*cut)
    return gain


def deal_out(own_key, own, number, rows, amount, top, most, lean):
    sequence = jax.random.permutation(own_key, amount)
    heavy_load, common = shares(amount, rows * top, most, lean, True), shares(amount, rows * top, most, lean, False)
    places = jnp.arange(amount)

    def named(sizes, rotation):
        used = int((sizes > 0).sum())
        fixed = max(1, used // 4)
        moved = fixed + (places - fixed + rotation * (used - fixed)) % max(1, amount - fixed)
        return jnp.zeros((amount,), jnp.int32).at[sequence[jnp.where(places < fixed, places, moved)]].set(jnp.asarray(sizes, jnp.int32))

    sizes = jnp.where(number % 4 == 0, named(heavy_load, number // 4), named(common, number - number // 4 - 1))
    mixed = jax.random.permutation(jax.random.fold_in(own, 3), amount)
    donor, taker = mixed[0:amount // 2 * 2:2], mixed[1:amount // 2 * 2:2]
    margin = jnp.minimum(sizes[donor] - 1, most - sizes[taker]) // 2
    margin = jnp.where((donor == sequence[0]) | (taker == sequence[0]) | (sizes[taker] == 0), 0, jnp.maximum(margin, 0))
    moved = jax.random.randint(jax.random.fold_in(own, 4), (amount // 2,), 0, 1 << 20) % (margin + 1)
    sizes = sizes.at[donor].add(-moved).at[taker].add(moved)
    members = jnp.searchsorted(jnp.cumsum(sizes), jnp.arange(rows * top), side="right").astype(jnp.int32)
    listing = members.reshape(top, rows).T
    listing = listing[jax.random.permutation(jax.random.fold_in(own, 1), rows)]
    rotation = jax.random.randint(jax.random.fold_in(own, 2), (rows, 1), 0, top)
    return jnp.take_along_axis(listing, (jnp.arange(top)[None, :] + rotation) % top, axis=1)


def shares(count, total, limit, lean, full):
    loads = [(1 << 20) // math.isqrt(rank ** lean) + 1 for rank in range(1, count + 1)]
    largest = limit if full else min(limit, max(-(-total // count), total * loads[0] // sum(loads)))
    least = 1 if total - largest >= count - 1 else 0
    counts, spare = [largest] + [least] * (count - 1), total - largest - least * (count - 1)
    while spare > 0:
        free = [i for i in range(1, count) if counts[i] < largest] or [i for i in range(1, count) if counts[i] < limit]
        whole, remaining = sum([loads[i] for i in free]), spare
        for i in free:
            more = min(limit - counts[i], max(1, remaining * loads[i] // whole), spare)
            counts[i] = counts[i] + more
            spare = spare - more
    return np.array(counts)


def centred(stream_key, extent, width, bound, cuts=(), kind=jnp.bfloat16):
    factor_of = block_scale(stream_key, extent, cuts, -0.22, 0.18) if cuts else 1.0
    result = jax.random.normal(stream_key, extent, jnp.float32) * width * factor_of
    return jnp.minimum(jnp.maximum(result, -bound), bound).astype(kind)


def setup_inputs(seed: int = 0) -> dict:
    arg_keys = jax.random.split(jax.random.key(seed), 5)
    grad_out = centred(arg_keys[0], (TOKENS, D), 0.03, 0.1875, ((0, 64), (1, 16)))
    expert_ids_keys = jax.random.split(jax.random.fold_in(arg_keys[1], 1), TOKENS // TOK_DEV)
    expert_ids_turns = jax.random.permutation(jax.random.fold_in(arg_keys[1], 3), TOKENS // TOK_DEV)
    expert_ids = jax.vmap(lambda own, number: deal_out(jax.random.fold_in(arg_keys[1], 2), own, number, TOK_DEV, EXPERTS, TOP, TOK_DEV // 2, 2))(expert_ids_keys, expert_ids_turns).reshape((TOKENS, TOP))
    route_gates = jnp.clip(0.1 + 0.9 * jax.random.uniform(arg_keys[2], (TOKENS, TOP), jnp.float32) ** block_scale(arg_keys[2], (TOKENS, TOP), ((0, 64),), -0.2, 0.2), 0.1, 1.0)
    saved_hidden = centred(arg_keys[3], (EXPERTS, SLOTS, FF), 1.0, 6.0, ((0, 8), (1, 8), (2, 16)))
    return dict(grad_out=grad_out, expert_ids=expert_ids, route_gates=route_gates, saved_hidden=saved_hidden)


def slot_table(expert_ids, route_gates, expert_count):
    routes = expert_ids.reshape(-1).astype(jnp.int32)
    weights = route_gates.reshape(-1)
    onehot = (routes[:, None] == jnp.arange(expert_count, dtype=jnp.int32)[None, :]).astype(jnp.int32)
    before = jnp.cumsum(onehot, axis=0) - onehot
    rank = jnp.sum(before * onehot, axis=1)
    target = jnp.where(rank < CAP, routes * CAP + rank, -1)
    match = jnp.arange(expert_count * CAP, dtype=jnp.int32)[:, None] == target[None, :]
    chosen = match.reshape(expert_count * CAP, -1, TOP).any(axis=2)
    slot_gate = jnp.sum(jnp.where(match, weights[None, :], jnp.zeros_like(weights)[None, :]), axis=1)
    return chosen.astype(jnp.bfloat16), slot_gate


def reference(grad_out, expert_ids, route_gates, saved_hidden):
    blocks = N_DP * EXPERTS
    grads = grad_out.reshape(blocks, TOK_DEV, D)
    ids = expert_ids.reshape(blocks, TOK_DEV, TOP)
    gates = route_gates.reshape(blocks, TOK_DEV, TOP)

    def one_block(items):
        grad_block, id_block, gate_block = items
        chosen, slot_gate = slot_table(id_block, gate_block, EXPERTS)
        picked = jnp.dot(chosen, grad_block, preferred_element_type=jnp.float32)
        return (picked * slot_gate[:, None]).astype(jnp.bfloat16).reshape(EXPERTS, CAP, D)

    slots = lax.map(one_block, (grads, ids, gates))
    slots = jnp.transpose(slots, (1, 0, 2, 3)).reshape(EXPERTS, blocks * CAP, D)

    def one_expert(items):
        hidden, expert_grads = items
        summed = lax.dot_general(hidden, expert_grads, (((0,), (0,)), ((), ())), preferred_element_type=jnp.float32)
        return summed.astype(jnp.bfloat16)

    return lax.map(one_expert, (saved_hidden, slots))
```

```python
import jax
import jax.numpy as jnp
from jax import lax
from jax.experimental import pallas as pl
from jax.experimental.pallas import tpu as pltpu
from jax.sharding import PartitionSpec as P

TOP = 2
CAP = 32
CORES = 2


def slot_table(expert_ids, route_gates, expert_count):
    routes = expert_ids.reshape(-1)
    weights = route_gates.reshape(-1)
    onehot = (routes[:, None] == jnp.arange(expert_count, dtype=jnp.int32)[None, :]).astype(
        jnp.int32
    )
    before = jnp.cumsum(onehot, axis=0) - onehot
    rank = jnp.sum(before * onehot, axis=1)
    target = jnp.where(rank < CAP, routes * CAP + rank, -1)
    match = jnp.arange(expert_count * CAP, dtype=jnp.int32)[:, None] == target[None, :]
    chosen = match.reshape(expert_count * CAP, -1, TOP).any(axis=2)
    slot_gate = jnp.sum(
        jnp.where(match, weights[None, :], jnp.zeros_like(weights)[None, :]), axis=1
    )
    return (chosen.astype(jnp.bfloat16), slot_gate)


def two_way_ring(first, second, axis, up, down, count):
    half = count // 2
    first_up, second_up, first_down, second_down = first, second, first, second
    pairs = []
    for step in range(1, half + 1):
        first_up = lax.ppermute(first_up, axis, up)
        second_down = lax.ppermute(second_down, axis, down)
        if step < half:
            second_up = lax.ppermute(second_up, axis, up)
            first_down = lax.ppermute(first_down, axis, down)
            pairs.append((-step, first_up, second_up))
            pairs.append((step, first_down, second_down))
        else:
            pairs.append((half, first_up, second_down))
    return pairs


def assemble_body(offsets, count, where_ref, own_ref, *rest):
    piece_refs, out_ref = rest[:-1], rest[-1]
    half = own_ref.shape[0] // 2

    def put(j, refs):
        row = pl.multiple_of(j * CAP, CAP)
        for k, ref in enumerate(refs):
            for i in range(ref.shape[0]):
                out_ref[k * half + i, pl.ds(row, CAP), :] = ref[i]

    me = where_ref[0]
    put(me, [own_ref])
    for n, offset in enumerate(offsets):
        put((me + offset) % count, piece_refs[2 * n : 2 * n + 2])


def matmul_body(offsets, count, where_ref, mine_ref, other_ref, hidden_ref, *rest):
    piece_refs, out_ref = rest[:-1], rest[-1]
    width = mine_ref.shape[2]
    me, core = where_ref[0], where_ref[1]
    total = [jnp.zeros((out_ref.shape[0], width), jnp.float32) for _ in range(2)]
    sources = [(0, hidden_ref[...])]
    for n, offset in enumerate(offsets):
        sources.append(
            (offset, jnp.concatenate([r[...] for r in piece_refs[2 * n : 2 * n + 2]], axis=0))
        )
    for offset, hidden in sources:
        i = (me + offset) % count
        for k, ref in enumerate((mine_ref, other_ref)):
            total[k] += lax.dot_general(
                hidden, ref[i], (((0,), (0,)), ((), ())), preferred_element_type=jnp.float32
            )
    for k in range(2):
        column = pl.multiple_of((core if k == 0 else 1 - core) * width, 128)
        out_ref[:, pl.ds(column, width)] = total[k].astype(out_ref.dtype)


def whole(array):
    return pl.BlockSpec(array.shape, lambda *_: (0,) * array.ndim)


def local(grad_out, expert_ids, route_gates, saved_hidden):
    data_count = lax.axis_size("dp")
    expert_count = lax.axis_size("expert")
    tensor_count = lax.axis_size("tensor")
    chips = tensor_count // CORES
    hidden = saved_hidden[0]
    rows, units = hidden.shape
    y_up = [(k, (k + 1) % data_count) for k in range(data_count)]
    y_down = [(k, (k - 1) % data_count) for k in range(data_count)]
    x_up = [(k, (k + CORES) % tensor_count) for k in range(tensor_count)]
    x_down = [(k, (k - CORES) % tensor_count) for k in range(tensor_count)]
    swap = [(k, k ^ 1) for k in range(tensor_count)]
    same_core = [[c + CORES * k for k in range(chips)] for c in range(CORES)]

    hidden_pairs = two_way_ring(
        hidden[: rows // 2], hidden[rows // 2 :], "dp", y_up, y_down, data_count
    )

    chosen, slot_gate = slot_table(expert_ids, route_gates, expert_count)
    picked = jnp.dot(chosen, grad_out, preferred_element_type=jnp.float32)
    slots = (picked * slot_gate[:, None]).astype(jnp.bfloat16)
    slots = slots.reshape(expert_count, CAP, grad_out.shape[1])
    slots = lax.all_to_all(slots, "expert", 0, 0, tiled=True)
    slots = lax.all_to_all(slots, "tensor", 0, 0, tiled=True, axis_index_groups=same_core)
    slots = lax.all_to_all(slots, "dp", 0, 0, tiled=True)
    width = slots.shape[2]
    slot_pairs = two_way_ring(
        slots[: data_count // 2], slots[data_count // 2 :], "tensor", x_up, x_down, chips
    )
    y = lax.axis_index("dp")
    t = lax.axis_index("tensor")
    x, core = t // CORES, t % CORES
    place = jnp.stack([x, core]).astype(jnp.int32)
    pieces = [p for pair in slot_pairs for p in pair[1:]]
    shape = jax.ShapeDtypeStruct((data_count, chips * CAP, width), jnp.bfloat16)
    smem = pl.BlockSpec(memory_space=pltpu.SMEM)
    mine = pl.pallas_call(
        lambda *refs: assemble_body([p[0] for p in slot_pairs], chips, *refs),
        out_shape=shape,
        in_specs=[smem] + [whole(a) for a in [slots, *pieces]],
        out_specs=whole(shape),
        name="assemble",
    )(place, slots, *pieces)
    other = lax.ppermute(mine, "tensor", swap)

    place = jnp.stack([y, core]).astype(jnp.int32)
    pieces = [p for pair in hidden_pairs for p in pair[1:]]
    block = 256
    out = pl.pallas_call(
        lambda *refs: matmul_body([p[0] for p in hidden_pairs], data_count, *refs),
        out_shape=jax.ShapeDtypeStruct((units, CORES * width), jnp.bfloat16),
        grid=(units // block,),
        in_specs=[smem, whole(mine), whole(other)]
        + [pl.BlockSpec((a.shape[0], block), lambda g: (0, g)) for a in [hidden, *pieces]],
        out_specs=pl.BlockSpec((block, CORES * width), lambda g: (g, 0)),
        name="matmul",
    )(place, mine, other, hidden, *pieces)
    return out[None]


def solution(mesh):
    in_specs = (
        P(("dp", "expert"), "tensor"),
        P(("dp", "expert"), None),
        P(("dp", "expert"), None),
        P("expert", "dp", "tensor"),
    )
    out_specs = P("expert", "tensor", "dp")
    return jax.shard_map(local, mesh=mesh, in_specs=in_specs, out_specs=out_specs, check_vma=False)
```

```python
import jax
import jax.numpy as jnp
from jax import lax
from jax.experimental import pallas as pl
from jax.experimental.pallas import tpu as pltpu
from jax.sharding import PartitionSpec as P

CAP = 32
CORES = 2


def select_body(experts, ids_ref, gates_ref, grads_ref, out_ref):
    tokens = ids_ref.shape[1]
    ids, gates = ids_ref[...], gates_ref[...]
    expert = lax.broadcasted_iota(jnp.int32, (experts, tokens), 0)
    named = jnp.zeros((experts, tokens), jnp.float32)
    gate = jnp.zeros((experts, tokens), jnp.float32)
    for k in range(ids_ref.shape[0]):
        hit = ids[k : k + 1, :] == expert
        named = jnp.where(hit, 1.0, named)
        gate = jnp.where(hit, gates[k : k + 1, :], gate)
    earlier = lax.broadcasted_iota(jnp.int32, (tokens, tokens), 0) < lax.broadcasted_iota(
        jnp.int32, (tokens, tokens), 1
    )
    rank = lax.dot_general(
        named.astype(jnp.bfloat16),
        earlier.astype(jnp.bfloat16),
        (((1,), (0,)), ((), ())),
        preferred_element_type=jnp.float32,
    )
    rank = jnp.where(named > 0, rank, -1.0).astype(jnp.int32)
    slot = lax.broadcasted_iota(jnp.int32, (CAP, tokens), 0)
    grads = grads_ref[...]
    for e in range(experts):
        hit = rank[e : e + 1, :] == slot
        weight = jnp.sum(jnp.where(hit, gate[e : e + 1, :], 0.0), axis=1, keepdims=True)
        chosen = jnp.where(hit, 1.0, 0.0).astype(jnp.bfloat16)
        picked = lax.dot_general(
            chosen, grads, (((1,), (0,)), ((), ())), preferred_element_type=jnp.float32
        )
        out_ref[e] = (picked * weight).astype(out_ref.dtype)


def one_way_pair(array, axis, up, down, count):
    half = count // 2
    below, above = array, array
    pieces = []
    for step in range(1, half + 1):
        below = lax.ppermute(below, axis, up)
        pieces.append((-step, below))
        if step < half:
            above = lax.ppermute(above, axis, down)
            pieces.append((step, above))
    return pieces


def assemble_body(offsets, count, where_ref, *refs):
    piece_refs, out_ref = refs[:-1], refs[-1]
    me = where_ref[0]
    for offset, ref in zip(offsets, piece_refs):
        row = ((me + offset) % count) * CAP
        for i in range(ref.shape[0]):
            start = pl.multiple_of(i * count * CAP + row, CAP)
            out_ref[pl.ds(start, CAP), :] = ref[i]


def matmul_body(where_ref, mine_ref, other_ref, hidden_ref, out_ref):
    width = mine_ref.shape[1]
    core = where_ref[0]
    hidden = hidden_ref[...]
    for k, ref in enumerate((mine_ref, other_ref)):
        total = lax.dot_general(
            hidden, ref[...], (((0,), (0,)), ((), ())), preferred_element_type=jnp.float32
        )
        column = pl.multiple_of((core if k == 0 else 1 - core) * width, 128)
        out_ref[:, pl.ds(column, width)] = total.astype(out_ref.dtype)


def whole(array):
    return pl.BlockSpec(array.shape, lambda *_: (0,) * array.ndim)


def in_vmem(array):
    return pltpu.with_memory_space_constraint(array, pltpu.VMEM)


def local(grad_out, expert_ids, route_gates, saved_hidden):
    data_count = lax.axis_size("dp")
    expert_count = lax.axis_size("expert")
    tensor_count = lax.axis_size("tensor")
    chips = tensor_count // CORES
    width = grad_out.shape[1]
    x_up = [(k, (k + CORES) % tensor_count) for k in range(tensor_count)]
    x_down = [(k, (k - CORES) % tensor_count) for k in range(tensor_count)]
    swap = [(k, k ^ 1) for k in range(tensor_count)]
    same_core = [[c + CORES * k for k in range(chips)] for c in range(CORES)]

    hidden = lax.all_gather(saved_hidden[0], "dp", axis=0, tiled=True)

    slots = pl.pallas_call(
        lambda *refs: select_body(expert_count, *refs),
        out_shape=pltpu.VMEM((expert_count, CAP, width), jnp.bfloat16),
        name="select",
    )(expert_ids.T, route_gates.T, grad_out)
    slots = lax.all_to_all(slots, "expert", 0, 0, tiled=True)
    slots = lax.all_to_all(slots, "tensor", 0, 0, tiled=True, axis_index_groups=same_core)
    slots = lax.all_to_all(slots, "dp", 0, 0, tiled=True)
    pieces = [(0, slots), *one_way_pair(slots, "tensor", x_up, x_down, chips)]

    t = lax.axis_index("tensor")
    smem = pl.BlockSpec(memory_space=pltpu.SMEM)
    vmem = pl.BlockSpec(memory_space=pltpu.VMEM)
    mine = pl.pallas_call(
        lambda *refs: assemble_body([p[0] for p in pieces], chips, *refs),
        out_shape=pltpu.VMEM((data_count * chips * CAP, width), jnp.bfloat16),
        in_specs=[smem] + [vmem] * len(pieces),
        out_specs=vmem,
        name="assemble",
    )((t // CORES).astype(jnp.int32)[None], *[in_vmem(p[1]) for p in pieces])
    other = lax.ppermute(mine, "tensor", swap)

    rows, units = hidden.shape
    block = 256
    out = pl.pallas_call(
        matmul_body,
        out_shape=jax.ShapeDtypeStruct((units, CORES * width), jnp.bfloat16),
        grid=(units // block,),
        in_specs=[smem, vmem, vmem, pl.BlockSpec((rows, block), lambda g: (0, g))],
        out_specs=pl.BlockSpec((block, CORES * width), lambda g: (g, 0)),
        name="matmul",
    )((t % CORES).astype(jnp.int32)[None], in_vmem(mine), in_vmem(other), hidden)
    return out[None]


def solution(mesh):
    in_specs = (
        P(("dp", "expert"), "tensor"),
        P(("dp", "expert"), None),
        P(("dp", "expert"), None),
        P("expert", "dp", "tensor"),
    )
    out_specs = P("expert", "tensor", "dp")
    return jax.shard_map(local, mesh=mesh, in_specs=in_specs, out_specs=out_specs, check_vma=False)
```

```python
import jax
import jax.numpy as jnp
from jax import lax
from jax.experimental import pallas as pl
from jax.experimental.pallas import tpu as pltpu
from jax.sharding import PartitionSpec as P


CAP = 32
CORES = 2


def select_body(experts, ids_ref, gates_ref, grads_ref, out_ref):
    tokens = ids_ref.shape[1]
    ids, gates = ids_ref[...], gates_ref[...]
    expert = lax.broadcasted_iota(jnp.int32, (experts, tokens), 0)
    named = jnp.zeros((experts, tokens), jnp.float32)
    gate = jnp.zeros((experts, tokens), jnp.float32)
    for k in range(ids_ref.shape[0]):
        hit = ids[k : k + 1, :] == expert
        named = jnp.where(hit, 1.0, named)
        gate = jnp.where(hit, gates[k : k + 1, :], gate)
    earlier = lax.broadcasted_iota(jnp.int32, (tokens, tokens), 0) < lax.broadcasted_iota(
        jnp.int32, (tokens, tokens), 1
    )
    rank = lax.dot_general(
        named.astype(jnp.bfloat16),
        earlier.astype(jnp.bfloat16),
        (((1,), (0,)), ((), ())),
        preferred_element_type=jnp.float32,
    )
    rank = jnp.where(named > 0, rank, -1.0).astype(jnp.int32)
    slot = lax.broadcasted_iota(jnp.int32, (CAP, tokens), 0)
    grads = grads_ref[...]
    for e in range(experts):
        hit = rank[e : e + 1, :] == slot
        weight = jnp.sum(jnp.where(hit, gate[e : e + 1, :], 0.0), axis=1, keepdims=True)
        chosen = jnp.where(hit, 1.0, 0.0).astype(jnp.bfloat16)
        picked = lax.dot_general(
            chosen, grads, (((1,), (0,)), ((), ())), preferred_element_type=jnp.float32
        )
        out_ref[e] = (picked * weight).astype(out_ref.dtype)


def part_body(at, in_ref, out_ref):
    out_ref[...] = in_ref[at : at + out_ref.shape[0], :]


def part(array, at, size):
    vmem = pl.BlockSpec(memory_space=pltpu.VMEM)
    return pl.pallas_call(
        lambda *refs: part_body(at, *refs),
        out_shape=pltpu.VMEM((size, array.shape[1]), array.dtype),
        in_specs=[vmem],
        out_specs=vmem,
        compiler_params=pltpu.CompilerParams(vmem_limit_bytes=1 << 20),
        name="part",
    )(in_vmem(array))


def copies_body(in_ref, out_ref):
    for k in range(out_ref.shape[0]):
        out_ref[k] = in_ref[...]


def hidden_ring(hidden, up, down, count):
    half, rows = count // 2, hidden.shape[0]
    below, above = hidden, hidden
    sources = []
    for step in range(1, half + 1):
        if step == half:
            below, above = part(below, 0, rows // 2), part(above, rows // 2, rows // 2)
        below = lax.ppermute(below, "dp", up)
        above = lax.ppermute(above, "dp", down)
        if step < half:
            sources += [(-step, [below]), (step, [above])]
        else:
            sources.append((half, [below, above]))
    return sources


def reorder(me, offsets, slots_ref, rows_ref):
    count, per_source = slots_ref.shape[1], slots_ref.shape[0] * CAP
    for n, offset in enumerate(offsets):
        i = (me + offset) % count
        for j in range(slots_ref.shape[0]):
            at = n * per_source + j * CAP
            rows_ref[at : at + CAP, :] = slots_ref[j, i]


def products(hidden_ref, rows_ref):
    block = hidden_ref.shape[1] // 4
    for g in range(4):
        units = slice(g * block, (g + 1) * block)
        yield units, lax.dot_general(
            hidden_ref[:, units],
            rows_ref[...],
            (((0,), (0,)), ((), ())),
            preferred_element_type=jnp.float32,
        )


def first_body(offsets, where_ref, slots_ref, *rest):
    piece_refs, out_ref, hidden_ref, rows_ref = rest[:-3], *rest[-3:]
    reorder(where_ref[0], offsets, slots_ref, rows_ref)
    at = 0
    for ref in piece_refs:
        hidden_ref[at : at + ref.shape[0], :] = ref[...]
        at += ref.shape[0]
    for units, total in products(hidden_ref, rows_ref):
        out_ref[units, :] = total.astype(out_ref.dtype)


def second_body(offsets, where_ref, slots_ref, hidden_ref, done_ref, out_ref, rows_ref):
    width, core = slots_ref.shape[-1], where_ref[1]
    reorder(where_ref[0], offsets, slots_ref, rows_ref)
    out_ref[:, pl.ds(pl.multiple_of(core * width, 128), width)] = done_ref[...]
    column = pl.multiple_of((1 - core) * width, 128)
    for units, total in products(hidden_ref, rows_ref):
        out_ref[units, pl.ds(column, width)] = total.astype(out_ref.dtype)


def in_vmem(array):
    return pltpu.with_memory_space_constraint(array, pltpu.VMEM)


def local(grad_out, expert_ids, route_gates, saved_hidden):
    data_count = lax.axis_size("dp")
    expert_count = lax.axis_size("expert")
    tensor_count = lax.axis_size("tensor")
    chips = tensor_count // CORES
    width = grad_out.shape[1]
    hidden = saved_hidden[0]
    rows, units = hidden.shape
    y_up = [(k, (k + 1) % data_count) for k in range(data_count)]
    y_down = [(k, (k - 1) % data_count) for k in range(data_count)]
    swap = [(k, k ^ 1) for k in range(tensor_count)]
    same_core = [[c + CORES * k for k in range(chips)] for c in range(CORES)]
    smem = pl.BlockSpec(memory_space=pltpu.SMEM)
    vmem = pl.BlockSpec(memory_space=pltpu.VMEM)

    sources = [(0, [hidden])] + hidden_ring(hidden, y_up, y_down, data_count)

    slots = pl.pallas_call(
        lambda *refs: select_body(expert_count, *refs),
        out_shape=pltpu.VMEM((expert_count, CAP, width), jnp.bfloat16),
        name="select",
    )(expert_ids.T, route_gates.T, grad_out)
    slots = lax.all_to_all(slots, "expert", 0, 0, tiled=True)
    slots = lax.all_to_all(slots, "tensor", 0, 0, tiled=True, axis_index_groups=same_core)
    slots = lax.all_to_all(slots, "dp", 0, 0, tiled=True)
    copies = pl.pallas_call(
        copies_body,
        out_shape=jax.ShapeDtypeStruct((chips, *slots.shape), slots.dtype),
        in_specs=[vmem],
        out_specs=vmem,
        compiler_params=pltpu.CompilerParams(vmem_limit_bytes=4 << 20),
        name="copies",
    )(in_vmem(slots))
    mine = lax.all_to_all(copies, "tensor", 0, 0, tiled=False, axis_index_groups=same_core)
    other = lax.ppermute(mine, "tensor", swap)

    place = jnp.stack([lax.axis_index("dp"), lax.axis_index("tensor") % CORES])
    place = place.astype(jnp.int32)
    offsets = [offset for offset, _ in sources]
    pieces = [p if abs(o) == 1 else in_vmem(p) for o, ps in sources for p in ps]
    taken = data_count * rows
    params = pltpu.CompilerParams(vmem_limit_bytes=14 << 20)
    scratch = [pltpu.VMEM((taken, width), jnp.bfloat16)]
    done, gathered = pl.pallas_call(
        lambda *refs: first_body(offsets, *refs),
        out_shape=(
            pltpu.VMEM((units, width), jnp.bfloat16),
            pltpu.VMEM((taken, units), jnp.bfloat16),
        ),
        in_specs=[smem] + [vmem] * (1 + len(pieces)),
        out_specs=(vmem, vmem),
        scratch_shapes=scratch,
        compiler_params=params,
        name="first",
    )(place, in_vmem(mine), *pieces)
    out = pl.pallas_call(
        lambda *refs: second_body(offsets, *refs),
        out_shape=jax.ShapeDtypeStruct((units, CORES * width), jnp.bfloat16),
        in_specs=[smem] + [vmem] * 3,
        out_specs=vmem,
        scratch_shapes=scratch,
        compiler_params=params,
        name="second",
    )(place, in_vmem(other), in_vmem(gathered), in_vmem(done))
    return out[None]


def solution(mesh):
    in_specs = (
        P(("dp", "expert"), "tensor"),
        P(("dp", "expert"), None),
        P(("dp", "expert"), None),
        P("expert", "dp", "tensor"),
    )
    out_specs = P("expert", "tensor", "dp")

    return jax.shard_map(local, mesh=mesh, in_specs=in_specs, out_specs=out_specs, check_vma=False)
```

```python
import jax
import jax.numpy as jnp
from jax import lax
from jax.experimental import pallas as pl
from jax.experimental.pallas import tpu as pltpu
from jax.sharding import PartitionSpec as P


CAP = 32
CORES = 2


def select_body(experts, ids_ref, gates_ref, grads_ref, out_ref):
    tokens = ids_ref.shape[1]
    ids, gates = ids_ref[...], gates_ref[...]
    expert = lax.broadcasted_iota(jnp.int32, (experts, tokens), 0)
    named = jnp.zeros((experts, tokens), jnp.float32)
    gate = jnp.zeros((experts, tokens), jnp.float32)
    for k in range(ids_ref.shape[0]):
        hit = ids[k : k + 1, :] == expert
        named = jnp.where(hit, 1.0, named)
        gate = jnp.where(hit, gates[k : k + 1, :], gate)
    earlier = lax.broadcasted_iota(jnp.int32, (tokens, tokens), 0) < lax.broadcasted_iota(
        jnp.int32, (tokens, tokens), 1
    )
    rank = lax.dot_general(
        named.astype(jnp.bfloat16),
        earlier.astype(jnp.bfloat16),
        (((1,), (0,)), ((), ())),
        preferred_element_type=jnp.float32,
    )
    rank = jnp.where(named > 0, rank, -1.0).astype(jnp.int32)
    slot = lax.broadcasted_iota(jnp.int32, (CAP, tokens), 0)
    grads = grads_ref[...]
    for e in range(experts):
        hit = rank[e : e + 1, :] == slot
        weight = jnp.sum(jnp.where(hit, gate[e : e + 1, :], 0.0), axis=1, keepdims=True)
        chosen = jnp.where(hit, 1.0, 0.0).astype(jnp.bfloat16)
        picked = lax.dot_general(
            chosen, grads, (((1,), (0,)), ((), ())), preferred_element_type=jnp.float32
        )
        out_ref[e] = (picked * weight).astype(out_ref.dtype)


def parts_body(in_ref, *out_refs):
    at = 0
    for ref in out_refs:
        ref[...] = in_ref[at : at + ref.shape[0]]
        at += ref.shape[0]


def two_halves(array):
    vmem = pl.BlockSpec(memory_space=pltpu.VMEM)
    half = pltpu.VMEM((array.shape[0] // 2, *array.shape[1:]), array.dtype)
    return pl.pallas_call(
        parts_body,
        out_shape=(half, half),
        in_specs=[vmem],
        out_specs=(vmem, vmem),
        compiler_params=pltpu.CompilerParams(vmem_limit_bytes=2 << 20),
        name="halves",
    )(in_vmem(array))


def twice_body(in_ref, out_ref):
    for k in range(2):
        out_ref[k] = in_ref[...]


def hidden_ring(hidden, up, down, count):
    half = count // 2
    below, above = hidden, hidden
    sources = []
    for step in range(1, half + 1):
        if step == half:
            below, above = two_halves(below)[0], two_halves(above)[1]
        below = lax.ppermute(below, "dp", up)
        above = lax.ppermute(above, "dp", down)
        if step < half:
            sources += [(-step, [below]), (step, [above])]
        else:
            sources.append((half, [below, above]))
    return sources


def assemble_body(count, where_ref, *refs):
    me, mine = where_ref[0], where_ref[1]
    own_ref, below_ref, above_ref, *far_refs, out_ref = refs
    groups = count // 2
    size = own_ref.shape[1] * own_ref.shape[2]
    for step, pieces in ((0, [own_ref]), (-1, [below_ref]), (1, [above_ref]), (2, far_refs)):
        row = ((mine + step) % groups) * size
        i = 0
        for ref in pieces:
            for k in range(ref.shape[0]):
                ahead = (i - me) % count
                place = jnp.where(
                    ahead <= count // 2,
                    2 * ahead - jnp.where(ahead == count // 2, 1, 0),
                    2 * (count - ahead) - 1,
                )
                for part in range(ref.shape[1]):
                    start = place * (groups * size) + row + part * CAP
                    out_ref[pl.ds(pl.multiple_of(start, CAP), CAP), :] = ref[k, part]
                i += 1


def products(hidden_ref, rows_ref):
    block = hidden_ref.shape[1] // 4
    for g in range(4):
        units = slice(g * block, (g + 1) * block)
        yield units, lax.dot_general(
            hidden_ref[:, units],
            rows_ref[...],
            (((0,), (0,)), ((), ())),
            preferred_element_type=jnp.float32,
        )


def first_body(rows_ref, *rest):
    piece_refs, out_ref, hidden_ref = rest[:-2], *rest[-2:]
    at = 0
    for ref in piece_refs:
        hidden_ref[at : at + ref.shape[0], :] = ref[...]
        at += ref.shape[0]
    for units, total in products(hidden_ref, rows_ref):
        out_ref[units, :] = total.astype(out_ref.dtype)


def second_body(where_ref, rows_ref, hidden_ref, done_ref, out_ref):
    width, core = rows_ref.shape[-1], where_ref[2]
    out_ref[:, pl.ds(pl.multiple_of(core * width, 128), width)] = done_ref[...]
    column = pl.multiple_of((1 - core) * width, 128)
    for units, total in products(hidden_ref, rows_ref):
        out_ref[units, pl.ds(column, width)] = total.astype(out_ref.dtype)


def in_vmem(array):
    return pltpu.with_memory_space_constraint(array, pltpu.VMEM)


def local(grad_out, expert_ids, route_gates, saved_hidden):
    data_count = lax.axis_size("dp")
    expert_count = lax.axis_size("expert")
    tensor_count = lax.axis_size("tensor")
    chips = tensor_count // CORES
    width = grad_out.shape[1]
    hidden = saved_hidden[0]
    rows, units = hidden.shape
    y_up = [(k, (k + 1) % data_count) for k in range(data_count)]
    y_down = [(k, (k - 1) % data_count) for k in range(data_count)]

    def shift(by):
        return [(k, (k + by) % tensor_count) for k in range(tensor_count)]

    swap = [(k, k ^ 1) for k in range(tensor_count)]
    same_core = [[c + CORES * k for k in range(chips)] for c in range(CORES)]
    smem = pl.BlockSpec(memory_space=pltpu.SMEM)
    vmem = pl.BlockSpec(memory_space=pltpu.VMEM)

    sources = [(0, [hidden])] + hidden_ring(hidden, y_up, y_down, data_count)

    slots = pl.pallas_call(
        lambda *refs: select_body(expert_count, *refs),
        out_shape=pltpu.VMEM((expert_count, CAP, width), jnp.bfloat16),
        name="select",
    )(expert_ids.T, route_gates.T, grad_out)
    slots = lax.all_to_all(slots, "expert", 0, 0, tiled=True)
    groups = chips // 2
    slots = pl.pallas_call(
        twice_body,
        out_shape=jax.ShapeDtypeStruct((2, *slots.shape), slots.dtype),
        in_specs=[vmem],
        out_specs=vmem,
        compiler_params=pltpu.CompilerParams(vmem_limit_bytes=2 << 20),
        name="twice",
    )(in_vmem(slots))
    slots = slots.reshape(chips, expert_count // groups, CAP, width)
    slots = lax.all_to_all(slots, "tensor", 0, 0, tiled=True, axis_index_groups=same_core)
    slots = lax.all_to_all(slots, "dp", 0, 0, tiled=True)
    lower, upper = two_halves(slots)
    below = lax.ppermute(slots, "tensor", shift(CORES))
    above = lax.ppermute(slots, "tensor", shift(-CORES))
    lower = lax.ppermute(lower, "tensor", shift(2 * CORES))
    upper = lax.ppermute(upper, "tensor", shift(-2 * CORES))

    t = lax.axis_index("tensor")
    place = jnp.stack([lax.axis_index("dp"), t // CORES % groups, t % CORES]).astype(jnp.int32)
    taken = data_count * rows
    mine = pl.pallas_call(
        lambda *refs: assemble_body(data_count, *refs),
        out_shape=pltpu.VMEM((taken, width), jnp.bfloat16),
        in_specs=[smem] + [vmem] * 5,
        out_specs=vmem,
        compiler_params=pltpu.CompilerParams(vmem_limit_bytes=4 << 20),
        name="assemble",
    )(place, *[in_vmem(p) for p in (slots, below, above, lower, upper)])
    other = lax.ppermute(mine, "tensor", swap)

    pieces = [p for _, ps in sources for p in ps]
    params = pltpu.CompilerParams(vmem_limit_bytes=14 << 20)
    done, gathered = pl.pallas_call(
        first_body,
        out_shape=(
            pltpu.VMEM((units, width), jnp.bfloat16),
            pltpu.VMEM((taken, units), jnp.bfloat16),
        ),
        in_specs=[vmem] * (1 + len(pieces)),
        out_specs=(vmem, vmem),
        compiler_params=params,
        name="first",
    )(in_vmem(mine), *pieces)
    out = pl.pallas_call(
        second_body,
        out_shape=jax.ShapeDtypeStruct((units, CORES * width), jnp.bfloat16),
        in_specs=[smem] + [vmem] * 3,
        out_specs=vmem,
        compiler_params=params,
        name="second",
    )(place, in_vmem(other), in_vmem(gathered), in_vmem(done))
    return out[None]


def solution(mesh):
    in_specs = (
        P(("dp", "expert"), "tensor"),
        P(("dp", "expert"), None),
        P(("dp", "expert"), None),
        P("expert", "dp", "tensor"),
    )
    out_specs = P("expert", "tensor", "dp")

    return jax.shard_map(local, mesh=mesh, in_specs=in_specs, out_specs=out_specs, check_vma=False)
```

```python
import jax
import jax.numpy as jnp
from jax import lax
from jax.experimental import pallas as pl
from jax.experimental.pallas import tpu as pltpu
from jax.sharding import PartitionSpec as P


CAP = 32
CORES = 2


def select_body(experts, ids_ref, gates_ref, grads_ref, out_ref):
    tokens = ids_ref.shape[1]
    ids, gates = ids_ref[...], gates_ref[...]
    expert = lax.broadcasted_iota(jnp.int32, (experts, tokens), 0)
    named = jnp.zeros((experts, tokens), jnp.float32)
    gate = jnp.zeros((experts, tokens), jnp.float32)
    for k in range(ids_ref.shape[0]):
        hit = ids[k : k + 1, :] == expert
        named = jnp.where(hit, 1.0, named)
        gate = jnp.where(hit, gates[k : k + 1, :], gate)
    earlier = lax.broadcasted_iota(jnp.int32, (tokens, tokens), 0) < lax.broadcasted_iota(
        jnp.int32, (tokens, tokens), 1
    )
    rank = lax.dot_general(
        named.astype(jnp.bfloat16),
        earlier.astype(jnp.bfloat16),
        (((1,), (0,)), ((), ())),
        preferred_element_type=jnp.float32,
    )
    rank = jnp.where(named > 0, rank, -1.0).astype(jnp.int32)
    slot = lax.broadcasted_iota(jnp.int32, (CAP, tokens), 0)
    grads = grads_ref[...]
    for e in range(experts):
        hit = rank[e : e + 1, :] == slot
        weight = jnp.sum(jnp.where(hit, gate[e : e + 1, :], 0.0), axis=1, keepdims=True)
        chosen = jnp.where(hit, 1.0, 0.0).astype(jnp.bfloat16)
        picked = lax.dot_general(
            chosen, grads, (((1,), (0,)), ((), ())), preferred_element_type=jnp.float32
        )
        out_ref[e] = (picked * weight).astype(out_ref.dtype)


def pick_body(where_ref, even_ref, odd_ref, out_ref):
    @pl.when(where_ref[2] == 0)
    def _():
        out_ref[...] = even_ref[...]

    @pl.when(where_ref[2] != 0)
    def _():
        out_ref[...] = odd_ref[...]


def pick(place, even, odd):
    vmem = pl.BlockSpec(memory_space=pltpu.VMEM)
    return pl.pallas_call(
        pick_body,
        out_shape=pltpu.VMEM(even.shape, even.dtype),
        in_specs=[pl.BlockSpec(memory_space=pltpu.SMEM), vmem, vmem],
        out_specs=vmem,
        compiler_params=pltpu.CompilerParams(vmem_limit_bytes=2 << 20),
        name="pick",
    )(place, in_vmem(even), in_vmem(odd))


def twice_body(in_ref, out_ref):
    for k in range(2):
        out_ref[k] = in_ref[...]


def hidden_ring(hidden, place, count, tensor_count):
    up = [(k, (k + 1) % count) for k in range(count)]
    down = [(k, (k - 1) % count) for k in range(count)]
    below, above, pieces = hidden, hidden, [hidden]
    for _ in range(1, count // 2):
        below = lax.ppermute(below, "dp", up)
        above = lax.ppermute(above, "dp", down)
        pieces += [below, above]
    across = [
        (y * tensor_count + t, (y + 1 - 2 * (t % CORES)) % count * tensor_count + t)
        for y in range(count)
        for t in range(tensor_count)
    ]
    last = pick(place, below, above)
    last = lax.ppermute(last, ("dp", "tensor"), across)
    return pieces + [last]


def assemble_body(count, where_ref, *refs):
    me, mine = where_ref[0], where_ref[1]
    own_ref, below_ref, above_ref, far_ref, out_ref = refs
    groups = count // 2
    size = own_ref.shape[1] * own_ref.shape[2]
    for step, ref in ((0, own_ref), (-1, below_ref), (1, above_ref), (2, far_ref)):
        row = ((mine + step) % groups) * size
        for i in range(count):
            ahead = (i - me) % count
            place = jnp.where(
                ahead <= count // 2,
                2 * ahead - jnp.where(ahead == count // 2, 1, 0),
                2 * (count - ahead) - 1,
            )
            for part in range(ref.shape[1]):
                start = place * (groups * size) + row + part * CAP
                out_ref[pl.ds(pl.multiple_of(start, CAP), CAP), :] = ref[i, part]


def products(hidden_ref, rows_ref):
    block = hidden_ref.shape[1] // 4
    for g in range(4):
        units = slice(g * block, (g + 1) * block)
        yield units, lax.dot_general(
            hidden_ref[:, units],
            rows_ref[...],
            (((0,), (0,)), ((), ())),
            preferred_element_type=jnp.float32,
        )


def first_body(rows_ref, *rest):
    piece_refs, out_ref, hidden_ref = rest[:-2], *rest[-2:]
    at = 0
    for ref in piece_refs:
        hidden_ref[at : at + ref.shape[0], :] = ref[...]
        at += ref.shape[0]
    for units, total in products(hidden_ref, rows_ref):
        out_ref[units, :] = total.astype(out_ref.dtype)


def second_body(where_ref, rows_ref, hidden_ref, done_ref, out_ref):
    width, core = rows_ref.shape[-1], where_ref[2]
    out_ref[:, pl.ds(pl.multiple_of(core * width, 128), width)] = done_ref[...]
    column = pl.multiple_of((1 - core) * width, 128)
    for units, total in products(hidden_ref, rows_ref):
        out_ref[units, pl.ds(column, width)] = total.astype(out_ref.dtype)


def in_vmem(array):
    return pltpu.with_memory_space_constraint(array, pltpu.VMEM)


def local(grad_out, expert_ids, route_gates, saved_hidden):
    data_count = lax.axis_size("dp")
    expert_count = lax.axis_size("expert")
    tensor_count = lax.axis_size("tensor")
    chips = tensor_count // CORES
    width = grad_out.shape[1]
    hidden = saved_hidden[0]
    rows, units = hidden.shape
    groups = chips // 2

    def shift(*by):
        return [(k, (k + by[k % len(by)]) % tensor_count) for k in range(tensor_count)]

    swap = [(k, k ^ 1) for k in range(tensor_count)]
    same_core = [[c + CORES * k for k in range(chips)] for c in range(CORES)]
    smem = pl.BlockSpec(memory_space=pltpu.SMEM)
    vmem = pl.BlockSpec(memory_space=pltpu.VMEM)

    t = lax.axis_index("tensor")
    place = jnp.stack([lax.axis_index("dp"), t // CORES % groups, t % CORES]).astype(jnp.int32)
    pieces = hidden_ring(hidden, place, data_count, tensor_count)

    slots = pl.pallas_call(
        lambda *refs: select_body(expert_count, *refs),
        out_shape=pltpu.VMEM((expert_count, CAP, width), jnp.bfloat16),
        name="select",
    )(expert_ids.T, route_gates.T, grad_out)
    slots = lax.all_to_all(slots, "expert", 0, 0, tiled=True)
    slots = pl.pallas_call(
        twice_body,
        out_shape=jax.ShapeDtypeStruct((2, *slots.shape), slots.dtype),
        in_specs=[vmem],
        out_specs=vmem,
        compiler_params=pltpu.CompilerParams(vmem_limit_bytes=2 << 20),
        name="twice",
    )(in_vmem(slots))
    slots = slots.reshape(chips, expert_count // groups, CAP, width)
    slots = lax.all_to_all(slots, "tensor", 0, 0, tiled=True, axis_index_groups=same_core)
    slots = lax.all_to_all(slots, "dp", 0, 0, tiled=True)
    below = lax.ppermute(slots, "tensor", shift(CORES))
    above = lax.ppermute(slots, "tensor", shift(-CORES))
    far = lax.ppermute(slots, "tensor", shift(2 * CORES, -2 * CORES))

    taken = data_count * rows
    mine = pl.pallas_call(
        lambda *refs: assemble_body(data_count, *refs),
        out_shape=pltpu.VMEM((taken, width), jnp.bfloat16),
        in_specs=[smem] + [vmem] * 4,
        out_specs=vmem,
        compiler_params=pltpu.CompilerParams(vmem_limit_bytes=4 << 20),
        name="assemble",
    )(place, *[in_vmem(p) for p in (slots, below, above, far)])
    other = lax.ppermute(mine, "tensor", swap)

    params = pltpu.CompilerParams(vmem_limit_bytes=14 << 20)
    done, gathered = pl.pallas_call(
        first_body,
        out_shape=(
            pltpu.VMEM((units, width), jnp.bfloat16),
            pltpu.VMEM((taken, units), jnp.bfloat16),
        ),
        in_specs=[vmem] * (1 + len(pieces)),
        out_specs=(vmem, vmem),
        compiler_params=params,
        name="first",
    )(in_vmem(mine), *pieces)
    out = pl.pallas_call(
        second_body,
        out_shape=jax.ShapeDtypeStruct((units, CORES * width), jnp.bfloat16),
        in_specs=[smem] + [vmem] * 3,
        out_specs=vmem,
        compiler_params=params,
        name="second",
    )(place, in_vmem(other), in_vmem(gathered), in_vmem(done))
    return out[None]


def solution(mesh):
    in_specs = (
        P(("dp", "expert"), "tensor"),
        P(("dp", "expert"), None),
        P(("dp", "expert"), None),
        P("expert", "dp", "tensor"),
    )
    out_specs = P("expert", "tensor", "dp")

    return jax.shard_map(local, mesh=mesh, in_specs=in_specs, out_specs=out_specs, check_vma=False)
```

```python
import jax
import jax.numpy as jnp
from jax import lax
from jax.experimental import pallas as pl
from jax.experimental.pallas import tpu as pltpu
from jax.sharding import PartitionSpec as P


CAP = 32
CORES = 2


def select_body(experts, ids_ref, gates_ref, grads_ref, out_ref):
    tokens = ids_ref.shape[1]
    ids, gates = ids_ref[...], gates_ref[...]
    expert = lax.broadcasted_iota(jnp.int32, (experts, tokens), 0)
    named = jnp.zeros((experts, tokens), jnp.float32)
    gate = jnp.zeros((experts, tokens), jnp.float32)
    for k in range(ids_ref.shape[0]):
        hit = ids[k : k + 1, :] == expert
        named = jnp.where(hit, 1.0, named)
        gate = jnp.where(hit, gates[k : k + 1, :], gate)
    earlier = lax.broadcasted_iota(jnp.int32, (tokens, tokens), 0) < lax.broadcasted_iota(
        jnp.int32, (tokens, tokens), 1
    )
    rank = lax.dot_general(
        named.astype(jnp.bfloat16),
        earlier.astype(jnp.bfloat16),
        (((1,), (0,)), ((), ())),
        preferred_element_type=jnp.float32,
    )
    rank = jnp.where(named > 0, rank, -1.0).astype(jnp.int32)
    slot = lax.broadcasted_iota(jnp.int32, (CAP, tokens), 0)
    grads = grads_ref[...]
    for e in range(experts):
        hit = rank[e : e + 1, :] == slot
        weight = jnp.sum(jnp.where(hit, gate[e : e + 1, :], 0.0), axis=1, keepdims=True)
        chosen = jnp.where(hit, 1.0, 0.0).astype(jnp.bfloat16)
        picked = lax.dot_general(
            chosen, grads, (((1,), (0,)), ((), ())), preferred_element_type=jnp.float32
        )
        out_ref[e] = (picked * weight).astype(out_ref.dtype)


def pick_body(where_ref, even_ref, odd_ref, out_ref):
    @pl.when(where_ref[2] == 0)
    def _():
        out_ref[...] = even_ref[...]

    @pl.when(where_ref[2] != 0)
    def _():
        out_ref[...] = odd_ref[...]


def pick(place, even, odd):
    vmem = pl.BlockSpec(memory_space=pltpu.VMEM)
    return pl.pallas_call(
        pick_body,
        out_shape=pltpu.VMEM(even.shape, even.dtype),
        in_specs=[pl.BlockSpec(memory_space=pltpu.SMEM), vmem, vmem],
        out_specs=vmem,
        compiler_params=pltpu.CompilerParams(vmem_limit_bytes=2 << 20),
        name="pick",
    )(place, in_vmem(even), in_vmem(odd))


def twice_body(in_ref, out_ref):
    for k in range(2):
        out_ref[k] = in_ref[...]


def hidden_ring(hidden, place, count, tensor_count):
    up = [(k, (k + 1) % count) for k in range(count)]
    down = [(k, (k - 1) % count) for k in range(count)]
    below, above, pieces = hidden, hidden, [hidden]
    for _ in range(1, count // 2):
        below = lax.ppermute(below, "dp", up)
        above = lax.ppermute(above, "dp", down)
        pieces += [below, above]
    across = [
        (y * tensor_count + t, (y + 1 - 2 * (t % CORES)) % count * tensor_count + t)
        for y in range(count)
        for t in range(tensor_count)
    ]
    last = pick(place, below, above)
    last = lax.ppermute(last, ("dp", "tensor"), across)
    return pieces + [last]


def assemble_body(count, where_ref, *refs):
    me, mine = where_ref[0], where_ref[1]
    own_ref, below_ref, above_ref, far_ref, out_ref = refs
    groups = count // 2
    size = own_ref.shape[1] * own_ref.shape[2]
    for step, ref in ((0, own_ref), (-1, below_ref), (1, above_ref), (2, far_ref)):
        row = ((mine + step) % groups) * size
        for i in range(count):
            ahead = (i - me) % count
            place = jnp.where(
                ahead <= count // 2,
                2 * ahead - jnp.where(ahead == count // 2, 1, 0),
                2 * (count - ahead) - 1,
            )
            for part in range(ref.shape[1]):
                start = place * (groups * size) + row + part * CAP
                out_ref[pl.ds(pl.multiple_of(start, CAP), CAP), :] = ref[i, part]


def products(hidden_ref, rows_ref):
    block = hidden_ref.shape[1] // 4
    for g in range(4):
        units = slice(g * block, (g + 1) * block)
        yield units, lax.dot_general(
            hidden_ref[:, units],
            rows_ref[...],
            (((0,), (0,)), ((), ())),
            preferred_element_type=jnp.float32,
        )


def first_body(rows_ref, *rest):
    piece_refs, out_ref, hidden_ref = rest[:-2], *rest[-2:]
    at = 0
    for ref in piece_refs:
        hidden_ref[at : at + ref.shape[0], :] = ref[...]
        at += ref.shape[0]
    for units, total in products(hidden_ref, rows_ref):
        out_ref[units, :] = total.astype(out_ref.dtype)


def second_body(where_ref, rows_ref, hidden_ref, done_ref, out_ref, block_ref, sems):
    width, core = rows_ref.shape[-1], where_ref[2]
    own = pl.ds(pl.multiple_of(core * width, 128), width)
    rest = pl.ds(pl.multiple_of((1 - core) * width, 128), width)
    copies = [pltpu.make_async_copy(done_ref, out_ref.at[:, own], sems.at[0])]
    copies[0].start()
    for units, total in products(hidden_ref, rows_ref):
        block_ref[units, :] = total.astype(block_ref.dtype)
        copies.append(
            pltpu.make_async_copy(
                block_ref.at[units], out_ref.at[units, rest], sems.at[len(copies)]
            )
        )
        copies[-1].start()
    for copy in copies:
        copy.wait()


def in_vmem(array):
    return pltpu.with_memory_space_constraint(array, pltpu.VMEM)


def in_hbm(array):
    return pltpu.with_memory_space_constraint(array, pltpu.HBM)


def local(grad_out, expert_ids, route_gates, saved_hidden):
    data_count = lax.axis_size("dp")
    expert_count = lax.axis_size("expert")
    tensor_count = lax.axis_size("tensor")
    chips = tensor_count // CORES
    width = grad_out.shape[1]
    hidden = saved_hidden[0]
    rows, units = hidden.shape
    groups = chips // 2

    def shift(*by):
        return [(k, (k + by[k % len(by)]) % tensor_count) for k in range(tensor_count)]

    swap = [(k, k ^ 1) for k in range(tensor_count)]
    same_core = [[c + CORES * k for k in range(chips)] for c in range(CORES)]
    smem = pl.BlockSpec(memory_space=pltpu.SMEM)
    vmem = pl.BlockSpec(memory_space=pltpu.VMEM)

    t = lax.axis_index("tensor")
    place = jnp.stack([lax.axis_index("dp"), t // CORES % groups, t % CORES]).astype(jnp.int32)
    pieces = hidden_ring(hidden, place, data_count, tensor_count)

    slots = pl.pallas_call(
        lambda *refs: select_body(expert_count, *refs),
        out_shape=pltpu.VMEM((expert_count, CAP, width), jnp.bfloat16),
        name="select",
    )(expert_ids.T, route_gates.T, grad_out)
    slots = lax.all_to_all(slots, "expert", 0, 0, tiled=True)
    slots = pl.pallas_call(
        twice_body,
        out_shape=jax.ShapeDtypeStruct((2, *slots.shape), slots.dtype),
        in_specs=[vmem],
        out_specs=vmem,
        compiler_params=pltpu.CompilerParams(vmem_limit_bytes=2 << 20),
        name="twice",
    )(in_vmem(slots))
    slots = slots.reshape(chips, expert_count // groups, CAP, width)
    slots = lax.all_to_all(slots, "tensor", 0, 0, tiled=True, axis_index_groups=same_core)
    slots = lax.all_to_all(slots, "dp", 0, 0, tiled=True)
    below = lax.ppermute(slots, "tensor", shift(CORES))
    above = lax.ppermute(slots, "tensor", shift(-CORES))
    far = lax.ppermute(slots, "tensor", shift(2 * CORES, -2 * CORES))

    taken = data_count * rows
    mine = pl.pallas_call(
        lambda *refs: assemble_body(data_count, *refs),
        out_shape=pltpu.VMEM((taken, width), jnp.bfloat16),
        in_specs=[smem] + [vmem] * 4,
        out_specs=vmem,
        compiler_params=pltpu.CompilerParams(vmem_limit_bytes=4 << 20),
        name="assemble",
    )(place, *[in_vmem(p) for p in (slots, below, above, far)])
    other = lax.ppermute(mine, "tensor", swap)

    params = pltpu.CompilerParams(vmem_limit_bytes=14 << 20)
    done, gathered = pl.pallas_call(
        first_body,
        out_shape=(
            pltpu.VMEM((units, width), jnp.bfloat16),
            pltpu.VMEM((taken, units), jnp.bfloat16),
        ),
        in_specs=[vmem] * (1 + len(pieces)),
        out_specs=(vmem, vmem),
        compiler_params=params,
        name="first",
    )(in_vmem(mine), *[in_hbm(p) if n in (1, 2, 3) else p for n, p in enumerate(pieces)])
    out = pl.pallas_call(
        second_body,
        out_shape=jax.ShapeDtypeStruct((units, CORES * width), jnp.bfloat16),
        in_specs=[smem] + [vmem] * 3,
        out_specs=pl.BlockSpec(memory_space=pl.ANY),
        scratch_shapes=[pltpu.VMEM((units, width), jnp.bfloat16), pltpu.SemaphoreType.DMA((5,))],
        compiler_params=params,
        name="second",
    )(place, in_vmem(other), in_vmem(gathered), in_vmem(done))
    return out[None]


def solution(mesh):
    in_specs = (
        P(("dp", "expert"), "tensor"),
        P(("dp", "expert"), None),
        P(("dp", "expert"), None),
        P("expert", "dp", "tensor"),
    )
    out_specs = P("expert", "tensor", "dp")

    return jax.shard_map(local, mesh=mesh, in_specs=in_specs, out_specs=out_specs, check_vma=False)
```

```python
import jax
import jax.numpy as jnp
from jax import lax
from jax.experimental import pallas as pl
from jax.experimental.pallas import tpu as pltpu
from jax.sharding import PartitionSpec as P


CAP = 32
CORES = 2


def select_body(experts, ids_ref, gates_ref, grads_ref, out_ref):
    tokens = ids_ref.shape[1]
    ids, gates = ids_ref[...], gates_ref[...]
    expert = lax.broadcasted_iota(jnp.int32, (experts, tokens), 0)
    named = jnp.zeros((experts, tokens), jnp.float32)
    gate = jnp.zeros((experts, tokens), jnp.float32)
    for k in range(ids_ref.shape[0]):
        hit = ids[k : k + 1, :] == expert
        named = jnp.where(hit, 1.0, named)
        gate = jnp.where(hit, gates[k : k + 1, :], gate)
    earlier = lax.broadcasted_iota(jnp.int32, (tokens, tokens), 0) < lax.broadcasted_iota(
        jnp.int32, (tokens, tokens), 1
    )
    rank = lax.dot_general(
        named.astype(jnp.bfloat16),
        earlier.astype(jnp.bfloat16),
        (((1,), (0,)), ((), ())),
        preferred_element_type=jnp.float32,
    )
    rank = jnp.where(named > 0, rank, -1.0).astype(jnp.int32)
    slot = lax.broadcasted_iota(jnp.int32, (CAP, tokens), 0)
    grads = grads_ref[...]
    for e in range(experts):
        hit = rank[e : e + 1, :] == slot
        weight = jnp.sum(jnp.where(hit, gate[e : e + 1, :], 0.0), axis=1, keepdims=True)
        chosen = jnp.where(hit, 1.0, 0.0).astype(jnp.bfloat16)
        picked = lax.dot_general(
            chosen, grads, (((1,), (0,)), ((), ())), preferred_element_type=jnp.float32
        )
        out_ref[e] = (picked * weight).astype(out_ref.dtype)


def pick_body(even_ref, odd_ref, out_ref):
    core = lax.axis_index("tensor") % CORES

    @pl.when(core == 0)
    def _():
        out_ref[...] = even_ref[...]

    @pl.when(core != 0)
    def _():
        out_ref[...] = odd_ref[...]


def pick(even, odd):
    vmem = pl.BlockSpec(memory_space=pltpu.VMEM)
    return pl.pallas_call(
        pick_body,
        out_shape=pltpu.VMEM(even.shape, even.dtype),
        in_specs=[vmem, vmem],
        out_specs=vmem,
        compiler_params=pltpu.CompilerParams(vmem_limit_bytes=2 << 20),
        name="pick",
    )(in_vmem(even), in_vmem(odd))


def twice_body(in_ref, out_ref):
    for k in range(2):
        out_ref[k] = in_ref[...]


def hidden_ring(hidden, count, tensor_count):
    up = [(k, (k + 1) % count) for k in range(count)]
    down = [(k, (k - 1) % count) for k in range(count)]
    below, above, pieces = hidden, hidden, [hidden]
    for _ in range(1, count // 2):
        below = lax.ppermute(below, "dp", up)
        above = lax.ppermute(above, "dp", down)
        pieces += [below, above]
    across = [
        (y * tensor_count + t, (y + 1 - 2 * (t % CORES)) % count * tensor_count + t)
        for y in range(count)
        for t in range(tensor_count)
    ]
    last = pick(below, above)
    last = lax.ppermute(last, ("dp", "tensor"), across)
    return pieces + [last]


def assemble_body(count, *refs):
    me, chip = lax.axis_index("dp"), lax.axis_index("tensor") // CORES
    own_ref, below_ref, above_ref, far_ref, out_ref = refs
    groups = count // 2
    size = own_ref.shape[1] * own_ref.shape[2]
    for step, ref in ((0, own_ref), (-1, below_ref), (1, above_ref), (2, far_ref)):
        row = ((chip + step) % groups) * size
        for i in range(count):
            ahead = (i - me) % count
            place = jnp.where(
                ahead <= count // 2,
                2 * ahead - jnp.where(ahead == count // 2, 1, 0),
                2 * (count - ahead) - 1,
            )
            for part in range(ref.shape[1]):
                start = place * (groups * size) + row + part * CAP
                out_ref[pl.ds(pl.multiple_of(start, CAP), CAP), :] = ref[i, part]


def product(hidden, rows):
    return lax.dot_general(
        hidden, rows, (((0,), (0,)), ((), ())), preferred_element_type=jnp.float32
    )


def blocks(size):
    return [slice(g * size // 4, (g + 1) * size // 4) for g in range(4)]


def first_body(rows_ref, *rest):
    piece_refs, part_ref, hidden_ref = rest[:-2], *rest[-2:]
    at = 0
    for ref in piece_refs:
        hidden_ref[at : at + ref.shape[0], :] = ref[...]
        at += ref.shape[0]
    for units in blocks(part_ref.shape[0]):
        part_ref[units, :] = product(hidden_ref[:, units], rows_ref[:at, :])


def second_body(
    mine_ref, other_ref, hidden_ref, last_ref, part_ref, out_ref, own_ref, rest_ref, sems
):
    width, core = mine_ref.shape[-1], lax.axis_index("tensor") % CORES
    early = hidden_ref.shape[0]
    columns = [pl.ds(pl.multiple_of(c * width, 128), width) for c in (core, 1 - core)]
    copies = []

    def send(ref, units, column):
        copies.append(
            pltpu.make_async_copy(
                ref.at[units], out_ref.at[units, column], sems.at[len(copies)]
            )
        )
        copies[-1].start()

    for units in blocks(part_ref.shape[0]):
        total = part_ref[units, :] + product(last_ref[:, units], mine_ref[early:, :])
        own_ref[units, :] = total.astype(own_ref.dtype)
        send(own_ref, units, columns[0])
    for units in blocks(part_ref.shape[0]):
        total = product(hidden_ref[:, units], other_ref[:early, :])
        total += product(last_ref[:, units], other_ref[early:, :])
        rest_ref[units, :] = total.astype(rest_ref.dtype)
        send(rest_ref, units, columns[1])
    for copy in copies:
        copy.wait()


def in_vmem(array):
    return pltpu.with_memory_space_constraint(array, pltpu.VMEM)


def local(grad_out, expert_ids, route_gates, saved_hidden):
    data_count = lax.axis_size("dp")
    expert_count = lax.axis_size("expert")
    tensor_count = lax.axis_size("tensor")
    chips = tensor_count // CORES
    width = grad_out.shape[1]
    hidden = saved_hidden[0]
    rows, units = hidden.shape
    groups = chips // 2

    def shift(*by):
        return [(k, (k + by[k % len(by)]) % tensor_count) for k in range(tensor_count)]

    swap = [(k, k ^ 1) for k in range(tensor_count)]
    same_core = [[c + CORES * k for k in range(chips)] for c in range(CORES)]
    vmem = pl.BlockSpec(memory_space=pltpu.VMEM)

    pieces = hidden_ring(hidden, data_count, tensor_count)

    slots = pl.pallas_call(
        lambda *refs: select_body(expert_count, *refs),
        out_shape=pltpu.VMEM((expert_count, CAP, width), jnp.bfloat16),
        name="select",
    )(expert_ids.T, route_gates.T, grad_out)
    slots = lax.all_to_all(slots, "expert", 0, 0, tiled=True)
    slots = pl.pallas_call(
        twice_body,
        out_shape=jax.ShapeDtypeStruct((2, *slots.shape), slots.dtype),
        in_specs=[vmem],
        out_specs=vmem,
        compiler_params=pltpu.CompilerParams(vmem_limit_bytes=2 << 20),
        name="twice",
    )(in_vmem(slots))
    slots = slots.reshape(chips, expert_count // groups, CAP, width)
    slots = lax.all_to_all(slots, "tensor", 0, 0, tiled=True, axis_index_groups=same_core)
    slots = lax.all_to_all(slots, "dp", 0, 0, tiled=True)
    below = lax.ppermute(slots, "tensor", shift(CORES))
    above = lax.ppermute(slots, "tensor", shift(-CORES))
    far = lax.ppermute(slots, "tensor", shift(2 * CORES, -2 * CORES))

    taken = data_count * rows
    early = taken - rows
    mine = pl.pallas_call(
        lambda *refs: assemble_body(data_count, *refs),
        out_shape=pltpu.VMEM((taken, width), jnp.bfloat16),
        in_specs=[vmem] * 4,
        out_specs=vmem,
        compiler_params=pltpu.CompilerParams(vmem_limit_bytes=4 << 20),
        name="assemble",
    )(*[in_vmem(p) for p in (slots, below, above, far)])
    other = lax.ppermute(mine, "tensor", swap)

    params = pltpu.CompilerParams(vmem_limit_bytes=14 << 20)
    part, gathered = pl.pallas_call(
        first_body,
        out_shape=(
            pltpu.VMEM((units, width), jnp.float32),
            pltpu.VMEM((early, units), jnp.bfloat16),
        ),
        in_specs=[vmem] * len(pieces),
        out_specs=(vmem, vmem),
        compiler_params=params,
        name="first",
    )(in_vmem(mine), *pieces[:-1])
    out = pl.pallas_call(
        second_body,
        out_shape=jax.ShapeDtypeStruct((units, CORES * width), jnp.bfloat16),
        in_specs=[vmem] * 5,
        out_specs=pl.BlockSpec(memory_space=pl.ANY),
        scratch_shapes=[
            pltpu.VMEM((units, width), jnp.bfloat16),
            pltpu.VMEM((units, width), jnp.bfloat16),
            pltpu.SemaphoreType.DMA((8,)),
        ],
        compiler_params=params,
        name="second",
    )(*[in_vmem(a) for a in (mine, other, gathered, pieces[-1], part)])
    return out[None]


def solution(mesh):
    in_specs = (
        P(("dp", "expert"), "tensor"),
        P(("dp", "expert"), None),
        P(("dp", "expert"), None),
        P("expert", "dp", "tensor"),
    )
    out_specs = P("expert", "tensor", "dp")

    return jax.shard_map(local, mesh=mesh, in_specs=in_specs, out_specs=out_specs, check_vma=False)
```

```python
import jax
import jax.numpy as jnp
from jax import lax
from jax.experimental import pallas as pl
from jax.experimental.pallas import tpu as pltpu
from jax.sharding import PartitionSpec as P


CAP = 32
CORES = 2


def select_body(experts, ids_ref, gates_ref, grads_ref, out_ref):
    tokens = ids_ref.shape[1]
    ids, gates = ids_ref[...], gates_ref[...]
    expert = lax.broadcasted_iota(jnp.int32, (experts, tokens), 0)
    named = jnp.zeros((experts, tokens), jnp.float32)
    gate = jnp.zeros((experts, tokens), jnp.float32)
    for k in range(ids_ref.shape[0]):
        hit = ids[k : k + 1, :] == expert
        named = jnp.where(hit, 1.0, named)
        gate = jnp.where(hit, gates[k : k + 1, :], gate)
    earlier = lax.broadcasted_iota(jnp.int32, (tokens, tokens), 0) < lax.broadcasted_iota(
        jnp.int32, (tokens, tokens), 1
    )
    rank = lax.dot_general(
        named.astype(jnp.bfloat16),
        earlier.astype(jnp.bfloat16),
        (((1,), (0,)), ((), ())),
        preferred_element_type=jnp.float32,
    )
    rank = jnp.where(named > 0, rank, -1.0).astype(jnp.int32)
    slot = lax.broadcasted_iota(jnp.int32, (CAP, tokens), 0)
    grads = grads_ref[...]
    for e in range(experts):
        hit = rank[e : e + 1, :] == slot
        weight = jnp.sum(jnp.where(hit, gate[e : e + 1, :], 0.0), axis=1, keepdims=True)
        chosen = jnp.where(hit, 1.0, 0.0).astype(jnp.bfloat16)
        picked = lax.dot_general(
            chosen, grads, (((1,), (0,)), ((), ())), preferred_element_type=jnp.float32
        )
        out_ref[e] = (picked * weight).astype(out_ref.dtype)


def pick_body(even_ref, odd_ref, out_ref):
    core = lax.axis_index("tensor") % CORES

    @pl.when(core == 0)
    def _():
        out_ref[...] = even_ref[...]

    @pl.when(core != 0)
    def _():
        out_ref[...] = odd_ref[...]


def pick(even, odd):
    vmem = pl.BlockSpec(memory_space=pltpu.VMEM)
    return pl.pallas_call(
        pick_body,
        out_shape=pltpu.VMEM(even.shape, even.dtype),
        in_specs=[vmem, vmem],
        out_specs=vmem,
        compiler_params=pltpu.CompilerParams(vmem_limit_bytes=2 << 20),
        name="pick",
    )(in_vmem(even), in_vmem(odd))


def twice_body(in_ref, out_ref):
    for k in range(2):
        out_ref[k] = in_ref[...]


def hidden_ring(hidden, count, tensor_count):
    up = [(k, (k + 1) % count) for k in range(count)]
    down = [(k, (k - 1) % count) for k in range(count)]
    below, above, pieces = hidden, hidden, [hidden]
    for _ in range(1, count // 2):
        below = lax.ppermute(below, "dp", up)
        above = lax.ppermute(above, "dp", down)
        pieces += [below, above]
    across = [
        (y * tensor_count + t, (y + 1 - 2 * (t % CORES)) % count * tensor_count + t)
        for y in range(count)
        for t in range(tensor_count)
    ]
    last = pick(below, above)
    last = lax.ppermute(last, ("dp", "tensor"), across)
    return pieces + [last]


def assemble_body(count, *refs):
    me, chip = lax.axis_index("dp"), lax.axis_index("tensor") // CORES
    own_ref, below_ref, above_ref, far_ref, out_ref = refs
    groups = count // 2
    size = own_ref.shape[1] * own_ref.shape[2]
    for step, ref in ((0, own_ref), (-1, below_ref), (1, above_ref), (2, far_ref)):
        row = ((chip + step) % groups) * size
        for i in range(count):
            ahead = (i - me) % count
            place = jnp.where(
                ahead <= count // 2,
                2 * ahead - jnp.where(ahead == count // 2, 1, 0),
                2 * (count - ahead) - 1,
            )
            for part in range(ref.shape[1]):
                start = place * (groups * size) + row + part * CAP
                out_ref[pl.ds(pl.multiple_of(start, CAP), CAP), :] = ref[i, part]


def products(hidden_ref, rows_ref):
    block = hidden_ref.shape[1] // 4
    for g in range(4):
        units = slice(g * block, (g + 1) * block)
        yield units, lax.dot_general(
            hidden_ref[:, units],
            rows_ref[...],
            (((0,), (0,)), ((), ())),
            preferred_element_type=jnp.float32,
        )


def first_body(rows_ref, *rest):
    piece_refs, out_ref, hidden_ref = rest[:-2], *rest[-2:]
    at = 0
    for ref in piece_refs:
        hidden_ref[at : at + ref.shape[0], :] = ref[...]
        at += ref.shape[0]
    for units, total in products(hidden_ref, rows_ref):
        out_ref[units, :] = total.astype(out_ref.dtype)


def second_body(rows_ref, hidden_ref, done_ref, out_ref, block_ref, sems):
    width, core = rows_ref.shape[-1], lax.axis_index("tensor") % CORES
    own = pl.ds(pl.multiple_of(core * width, 128), width)
    rest = pl.ds(pl.multiple_of((1 - core) * width, 128), width)
    copies = [pltpu.make_async_copy(done_ref, out_ref.at[:, own], sems.at[0])]
    copies[0].start()
    for units, total in products(hidden_ref, rows_ref):
        block_ref[units, :] = total.astype(block_ref.dtype)
        copies.append(
            pltpu.make_async_copy(
                block_ref.at[units], out_ref.at[units, rest], sems.at[len(copies)]
            )
        )
        copies[-1].start()
    for copy in copies:
        copy.wait()


def in_vmem(array):
    return pltpu.with_memory_space_constraint(array, pltpu.VMEM)


def local(grad_out, expert_ids, route_gates, saved_hidden):
    data_count = lax.axis_size("dp")
    expert_count = lax.axis_size("expert")
    tensor_count = lax.axis_size("tensor")
    chips = tensor_count // CORES
    width = grad_out.shape[1]
    hidden = saved_hidden[0]
    rows, units = hidden.shape
    groups = chips // 2

    def shift(*by):
        return [(k, (k + by[k % len(by)]) % tensor_count) for k in range(tensor_count)]

    swap = [(k, k ^ 1) for k in range(tensor_count)]
    same_core = [[c + CORES * k for k in range(chips)] for c in range(CORES)]
    vmem = pl.BlockSpec(memory_space=pltpu.VMEM)

    pieces = hidden_ring(hidden, data_count, tensor_count)

    slots = pl.pallas_call(
        lambda *refs: select_body(expert_count, *refs),
        out_shape=pltpu.VMEM((expert_count, CAP, width), jnp.bfloat16),
        name="select",
    )(expert_ids.T, route_gates.T, grad_out)
    slots = lax.all_to_all(slots, "expert", 0, 0, tiled=True)
    slots = pl.pallas_call(
        twice_body,
        out_shape=jax.ShapeDtypeStruct((2, *slots.shape), slots.dtype),
        in_specs=[vmem],
        out_specs=vmem,
        compiler_params=pltpu.CompilerParams(vmem_limit_bytes=2 << 20),
        name="twice",
    )(in_vmem(slots))
    slots = slots.reshape(chips, expert_count // groups, CAP, width)
    slots = lax.all_to_all(slots, "tensor", 0, 0, tiled=True, axis_index_groups=same_core)
    slots = lax.all_to_all(slots, "dp", 0, 0, tiled=True)
    below = lax.ppermute(slots, "tensor", shift(CORES))
    above = lax.ppermute(slots, "tensor", shift(-CORES))
    far = lax.ppermute(slots, "tensor", shift(2 * CORES, -2 * CORES))

    taken = data_count * rows
    mine = pl.pallas_call(
        lambda *refs: assemble_body(data_count, *refs),
        out_shape=pltpu.VMEM((taken, width), jnp.bfloat16),
        in_specs=[vmem] * 4,
        out_specs=vmem,
        compiler_params=pltpu.CompilerParams(vmem_limit_bytes=4 << 20),
        name="assemble",
    )(*[in_vmem(p) for p in (slots, below, above, far)])
    other = lax.ppermute(mine, "tensor", swap)

    params = pltpu.CompilerParams(vmem_limit_bytes=14 << 20)
    done, gathered = pl.pallas_call(
        first_body,
        out_shape=(
            pltpu.VMEM((units, width), jnp.bfloat16),
            pltpu.VMEM((taken, units), jnp.bfloat16),
        ),
        in_specs=[vmem] * (1 + len(pieces)),
        out_specs=(vmem, vmem),
        compiler_params=params,
        name="first",
    )(in_vmem(mine), *pieces)
    out = pl.pallas_call(
        second_body,
        out_shape=jax.ShapeDtypeStruct((units, CORES * width), jnp.bfloat16),
        in_specs=[vmem] * 3,
        out_specs=pl.BlockSpec(memory_space=pl.ANY),
        scratch_shapes=[pltpu.VMEM((units, width), jnp.bfloat16), pltpu.SemaphoreType.DMA((5,))],
        compiler_params=params,
        name="second",
    )(in_vmem(other), in_vmem(gathered), in_vmem(done))
    return out[None]


def solution(mesh):
    in_specs = (
        P(("dp", "expert"), "tensor"),
        P(("dp", "expert"), None),
        P(("dp", "expert"), None),
        P("expert", "dp", "tensor"),
    )
    out_specs = P("expert", "tensor", "dp")

    return jax.shard_map(local, mesh=mesh, in_specs=in_specs, out_specs=out_specs, check_vma=False)
```
